32 devices in a mesh: exp: 2 (over core), seq: 8 (over z, y), tp: 2 (over x).
Axes of the slice: x: 2, y: 2, z: 4, core: 2. Of those that a mesh axis runs over, the one named last changes fastest.
Arguments:
- tokens: bfloat16 [2048, 1536], P(('exp', 'seq')), may hold values from -6 to 6
- targets: bfloat16 [2048, 1536], P(('exp', 'seq')), may hold values from -6 to 6
- attn_gain: float32 [1536], replicated, may hold values from 0.5 to 1.5
- wq: bfloat16 [1536, 1536], P(None, 'tp'), may hold values from -0.21875 to 0.21875
- wk: bfloat16 [1536, 512], P(None, 'tp'), may hold values from -0.15625 to 0.15625
- wv: bfloat16 [1536, 512], P(None, 'tp'), may hold values from -0.15625 to 0.15625
- wo: bfloat16 [1536, 1536], P('tp'), may hold values from -1.75 to 1.75
- moe_gain: float32 [1536], replicated, may hold values from 0.5 to 1.5
- router: bfloat16 [1536, 40], replicated, may hold values from -0.078125 to 0.078125
- w_gate: bfloat16 [40, 1536, 512], P('exp', None, 'tp'), may hold values from -0.15625 to 0.15625
- w_up: bfloat16 [40, 1536, 512], P('exp', None, 'tp'), may hold values from -0.15625 to 0.15625
- w_down: bfloat16 [40, 512, 1536], P('exp', 'tp'), may hold values from -1 to 1
- routes: int32 [2048, 8], P(('exp', 'seq')), may hold values from 0 to 39, all different within a row; in each aligned block of 128 rows (0 to 127, 128 to 255, ...) at most 32 rows name the same one
- lengths: int32 [2, 3], replicated, may hold values from 1 to 640, 1024 in all within a row
- prefix: int32 [2, 3], replicated, may hold values from 0 to 511
Outputs:
- layer_out: float32 [2048, 1536], P(('exp', 'seq'))
- input_grad: float32 [2048, 1536], P(('exp', 'seq'))
- attn_gain_grad: float32 [1536], replicated
- wq_grad: float32 [1536, 1536], P(None, 'tp')
- wk_grad: float32 [1536, 512], P(None, 'tp')
- wv_grad: float32 [1536, 512], P(None, 'tp')
- wo_grad: float32 [1536, 1536], P('tp')
- moe_gain_grad: float32 [1536], replicated
- router_grad: float32 [1536, 40], replicated
- gate_grad: float32 [40, 1536, 512], P('exp', 'seq', 'tp')
- up_grad: float32 [40, 1536, 512], P('exp', 'seq', 'tp')
- down_grad: float32 [40, 512, 1536], P('exp', 'tp', 'seq')
The draws below stay inside these ranges and needn't reach their ends.
Inputs may be any that keep to these rules, and one draw needn't show every extreme that they name: `routes`: in each aligned block of 128 rows no expert is named by more than 32 rows, and in some block one expert is named by exactly 32 rows. `lengths`: each row sums to 1024; its largest entry equals the maximum.
All inputs are finite; a program needn't handle non-finite values.
Results may differ from the reference program's by a relative error of at most 0.024.
Values may be sent and summed in bfloat16 or wider, within the bound.
A program may use at most 320 MiB of HBM per device.

```python
import math
import jax
import jax.numpy as jnp
import numpy as np
from jax import lax

MODEL_SIZE = 1536
QUERY_HEADS = 24
KEY_VALUE_HEADS = 8
HEAD_SIZE = 64
EXPERTS = 40
FF = 512
TOP = 8
TOK_DEV = 128
DOCS = 3
CAP = 32
PACK_TOKENS = 1024
PACK_COUNT = 2
TOKEN_TOTAL = 2048
N_TP = 2


def place_ends(entries, stream_key, low, high):
    extent = entries.shape
    place = [jax.random.randint(jax.random.fold_in(stream_key, axis), (), 0, extent[axis]) for axis in range(len(extent))]
    entries = entries.at[tuple(place)].set(low)
    longest = extent.index(max(extent))
    place[longest] = (place[longest] + 1) % extent[longest]
    return entries.at[tuple(place)].set(high)


def block_scale(stream_key, extent, pieces, smallest, top_value):
    def one(axis_at, shards_of):
        draws = jax.random.uniform(jax.random.fold_in(jax.random.fold_in(stream_key, 6), axis_at), (shards_of,), jnp.float32, smallest / len(pieces), top_value / len(pieces))
        return jnp.repeat(jnp.exp(draws), extent[axis_at] // shards_of).reshape((-1,) + (1,) * (len(extent) - axis_at - 1))

    gain = one(*pieces[0])
    for cut in pieces[1:]:
        gain = gain * one(*cut)
    return gain


def split_up(number_of, total, limit, slope):
    portions = [(1 << 20) // math.isqrt(grade ** slope) + 1 for grade in range(2, number_of + 1)]
    surplus, holding = total - limit - (number_of - 1), [1] * (number_of - 1)
    while surplus > 0:
        candidates = [i for i in range(number_of - 1) if holding[i] < limit]
        whole, left = sum([portions[i] for i in candidates]), surplus
        for i in candidates:
            addition = min(limit - holding[i], max(1, left * portions[i] // whole), surplus)
            holding[i] = holding[i] + addition
            surplus = surplus - addition
    return np.array([limit] + holding)


def ragged_sizes(stream_key, amount, total, limit, lean):
    if amount == 2:
        one = jax.random.randint(stream_key, (), max(1, total - limit), min(limit, total - 1) + 1)
        return jnp.stack([one, total - one])
    tallies = jnp.asarray(split_up(amount, total, limit, lean), jnp.int32)
    twos = (amount - 1) // 2
    donor, sink = tallies[1:1 + 2 * twos:2], tallies[2:2 + 2 * twos:2]
    room = jnp.minimum(donor - 1, limit - sink)
    passed = jax.random.randint(jax.random.fold_in(stream_key, 1), (twos,), 0, 1 << 20) % (room + 1)
    tallies = tallies.at[1:1 + 2 * twos:2].set(donor - passed).at[2:2 + 2 * twos:2].set(sink + passed)
    return tallies[jax.random.permutation(jax.random.fold_in(stream_key, 2), amount)]


def shared_out(stream_key, own, number, rows, count, top, bound, skew):
    order = jax.random.permutation(stream_key, count)
    heavy_load, ordinary = portions_of(count, rows * top, bound, skew, True), portions_of(count, rows * top, bound, skew, False)
    places = jnp.arange(count)

    def named(sizes, turn):
        used = int((sizes > 0).sum())
        fixed = max(1, used // 4)
        moved = fixed + (places - fixed + turn * (used - fixed)) % max(1, count - fixed)
        return jnp.zeros((count,), jnp.int32).at[order[jnp.where(places < fixed, places, moved)]].set(jnp.asarray(sizes, jnp.int32))

    sizes = jnp.where(number % 4 == 0, named(heavy_load, number // 4), named(ordinary, number - number // 4 - 1))
    mixed = jax.random.permutation(jax.random.fold_in(own, 3), count)
    source_of, receiver = mixed[0:count // 2 * 2:2], mixed[1:count // 2 * 2:2]
    slack = jnp.minimum(sizes[source_of] - 1, bound - sizes[receiver]) // 2
    slack = jnp.where((source_of == order[0]) | (receiver == order[0]) | (sizes[receiver] == 0), 0, jnp.maximum(slack, 0))
    moved = jax.random.randint(jax.random.fold_in(own, 4), (count // 2,), 0, 1 << 20) % (slack + 1)
    sizes = sizes.at[source_of].add(-moved).at[receiver].add(moved)
    items = jnp.searchsorted(jnp.cumsum(sizes), jnp.arange(rows * top), side="right").astype(jnp.int32)
    table = items.reshape(top, rows).T
    table = table[jax.random.permutation(jax.random.fold_in(own, 1), rows)]
    turn = jax.random.randint(jax.random.fold_in(own, 2), (rows, 1), 0, top)
    return jnp.take_along_axis(table, (jnp.arange(top)[None, :] + turn) % top, axis=1)


def portions_of(count, total, bound, lean, full):
    loads = [(1 << 20) // math.isqrt(standing ** lean) + 1 for standing in range(1, count + 1)]
    largest = bound if full else min(bound, max(-(-total // count), total * loads[0] // sum(loads)))
    least = 1 if total - largest >= count - 1 else 0
    counts, spare = [largest] + [least] * (count - 1), total - largest - least * (count - 1)
    while spare > 0:
        movable = [i for i in range(1, count) if counts[i] < largest] or [i for i in range(1, count) if counts[i] < bound]
        pool, budget = sum([loads[i] for i in movable]), spare
        for i in movable:
            addition = min(bound - counts[i], max(1, budget * loads[i] // pool), spare)
            counts[i] = counts[i] + addition
            spare = spare - addition
    return np.array(counts)


def bell_draw(rng, dims, scale, bound, pieces=(), kind=jnp.bfloat16):
    entries = scale * jax.random.normal(rng, dims, jnp.float32)
    if pieces:
        entries = entries * block_scale(rng, dims, pieces, -0.22, 0.18)
    return jnp.clip(entries, -bound, bound).astype(kind)


def setup_inputs(seed: int = 0) -> dict:
    streams_of = jax.random.split(jax.random.key(seed), 16)
    tokens = bell_draw(streams_of[0], (TOKEN_TOTAL, MODEL_SIZE), 1.0, 6.0, ((0, 16),))
    targets = bell_draw(streams_of[1], (TOKEN_TOTAL, MODEL_SIZE), 1.0, 6.0, ((0, 16),))
    attn_gain = jnp.clip(1.0 + 0.1 * jax.random.normal(streams_of[2], (MODEL_SIZE,), jnp.float32), 0.5, 1.5)
    wq = bell_draw(streams_of[3], (MODEL_SIZE, QUERY_HEADS * HEAD_SIZE), (MODEL_SIZE // 2) ** -0.5, 0.21875, ((1, 2),))
    wk = bell_draw(streams_of[4], (MODEL_SIZE, KEY_VALUE_HEADS * HEAD_SIZE), MODEL_SIZE ** -0.5, 0.15625, ((1, 2),))
    wv = bell_draw(streams_of[5], (MODEL_SIZE, KEY_VALUE_HEADS * HEAD_SIZE), MODEL_SIZE ** -0.5, 0.15625, ((1, 2),))
    wo = bell_draw(streams_of[6], (QUERY_HEADS * HEAD_SIZE, MODEL_SIZE), (max(1, QUERY_HEADS * HEAD_SIZE // 128)) ** -0.5, 1.75, ((0, 2),))
    moe_gain = jnp.clip(1.0 + 0.1 * jax.random.normal(streams_of[7], (MODEL_SIZE,), jnp.float32), 0.5, 1.5)
    router = bell_draw(streams_of[8], (MODEL_SIZE, EXPERTS), (MODEL_SIZE * 4) ** -0.5, 0.078125)
    w_gate = bell_draw(streams_of[9], (EXPERTS, MODEL_SIZE, FF), MODEL_SIZE ** -0.5, 0.15625, ((0, 2), (2, 2)))
    w_up = bell_draw(streams_of[10], (EXPERTS, MODEL_SIZE, FF), MODEL_SIZE ** -0.5, 0.15625, ((0, 2), (2, 2)))
    w_down = bell_draw(streams_of[11], (EXPERTS, FF, MODEL_SIZE), (FF // 16) ** -0.5, 1.0, ((0, 2), (1, 2)))
    routes_keys = jax.random.split(jax.random.fold_in(streams_of[12], 1), TOKEN_TOTAL // TOK_DEV)
    routes_turns = jax.random.permutation(jax.random.fold_in(streams_of[12], 3), TOKEN_TOTAL // TOK_DEV)
    routes = jax.vmap(lambda own, number: shared_out(jax.random.fold_in(streams_of[12], 2), own, number, TOK_DEV, EXPERTS, TOP, CAP, 1))(routes_keys, routes_turns).reshape((TOKEN_TOTAL, TOP))
    lengths = jax.vmap(lambda own: ragged_sizes(own, DOCS, PACK_TOKENS, PACK_TOKENS * 5 // 8, 2))(jax.random.split(streams_of[13], PACK_COUNT)).reshape((PACK_COUNT, DOCS)).astype(jnp.int32)
    prefix = place_ends(jax.random.randint(streams_of[14], (PACK_COUNT, DOCS), 0, PACK_TOKENS // 2), jax.random.fold_in(streams_of[14], 1), 0, (PACK_TOKENS // 2) - 1).astype(jnp.int32)
    return {"tokens": tokens, "targets": targets, "attn_gain": attn_gain, "wq": wq, "wk": wk, "wv": wv, "wo": wo, "moe_gain": moe_gain, "router": router, "w_gate": w_gate, "w_up": w_up, "w_down": w_down, "routes": routes, "lengths": lengths, "prefix": prefix}


@jax.custom_vjp
def lower_precision(v):
    return lax.optimization_barrier(v.astype(jnp.bfloat16)).astype(jnp.float32)

@jax.custom_vjp
def lower_backward(v):
    return v

def low_keep(v):
    return (lower_precision(v), None)

def low_pass(kept, grad):
    return (grad,)

def back_keep(v):
    return (v, None)

def back_low(kept, grad):
    return (lower_precision(grad),)
lower_precision.defvjp(low_keep, low_pass)
lower_backward.defvjp(back_keep, back_low)
eps = 1e-06
neg_big = -1e+30

def matrix_product_exact(first_mat, second_mat):
    return jnp.dot(first_mat, second_mat, precision=lax.Precision.HIGHEST)

def rotate(tensor, cosine, sine_tab):
    half_dim = tensor.shape[-1] // 2
    first_half = tensor[..., :half_dim]
    second_half = tensor[..., half_dim:]
    return jnp.concatenate([first_half * cosine - second_half * sine_tab, second_half * cosine + first_half * sine_tab], axis=-1)

def doc_layout(doc_lengths, prefix_lens, pack_len):
    doc_ends = jnp.cumsum(doc_lengths, axis=1).astype(jnp.int32)
    starts = (doc_ends - doc_lengths).astype(jnp.int32)
    places = jnp.arange(pack_len, dtype=jnp.int32)
    document_index = lax.optimization_barrier(jnp.sum((places[None, :, None] >= doc_ends[:, None, :]).astype(jnp.int32), axis=2)).astype(jnp.int32)
    inside_document = (places[None, :] - jnp.take_along_axis(starts, document_index, axis=1)).astype(jnp.int32)
    prefix_length = jnp.take_along_axis(prefix_lens, document_index, axis=1).astype(jnp.int32)
    return (document_index, inside_document, prefix_length)

def attend(element):
    query_matrix, key_matrix, value_matrix, document_index, inside_document, prefix_length = element
    scaling = 1.0 / math.sqrt(HEAD_SIZE)
    scores = lower_backward(jnp.einsum('qrd,kd->rqk', query_matrix, key_matrix, precision=lax.Precision.HIGHEST) * scaling)
    places = jnp.arange(PACK_TOKENS, dtype=jnp.int32)
    allowed = (document_index[:, None] == document_index[None, :]) & ((places[None, :] <= places[:, None]) | (inside_document[None, :] < prefix_length[:, None]))
    scores = jnp.where(allowed[None], scores, neg_big)
    weights = lower_precision(jax.nn.softmax(scores, axis=-1))
    return jnp.einsum('rqk,kd->qrd', weights, value_matrix, precision=lax.Precision.HIGHEST)

def expert(element):
    routed, gate_mat, up_mat, down_mat = element
    units = FF // N_TP
    summed = None
    for piece_index in range(N_TP):
        columns = slice(piece_index * units, (piece_index + 1) * units)
        inner_in = lower_backward(routed)
        gate_pre = lower_backward(matrix_product_exact(inner_in, gate_mat[:, columns]))
        up_pre = lower_backward(matrix_product_exact(inner_in, up_mat[:, columns]))
        hidden = lower_precision(jax.nn.silu(gate_pre) * up_pre)
        partial_term = lower_precision(lower_backward(matrix_product_exact(hidden, down_mat[columns, :])))
        summed = partial_term if summed is None else summed + partial_term
    return summed

def reference(tokens, targets, attn_gain, wq, wk, wv, wo, moe_gain, router, w_gate, w_up, w_down, routes, lengths, prefix):
    repeat_heads = QUERY_HEADS // KEY_VALUE_HEADS
    blocks = TOKEN_TOTAL // TOK_DEV
    prefix_eff = jnp.minimum(prefix, lengths - 1).astype(jnp.int32)
    document_index, inside_document, prefix_length = doc_layout(lengths, prefix_eff, PACK_TOKENS)
    frequency = jnp.exp(jnp.arange(HEAD_SIZE // 2, dtype=jnp.float32) * (-2.0 * math.log(10000.0) / HEAD_SIZE))
    angles = inside_document.reshape(TOKEN_TOTAL).astype(jnp.float32)[:, None, None] * frequency[None, None, :]
    cosine = jnp.cos(angles)
    sine_tab = jnp.sin(angles)
    document_repeated = jnp.repeat(document_index, KEY_VALUE_HEADS, axis=0)
    position_repeated = jnp.repeat(inside_document, KEY_VALUE_HEADS, axis=0)
    prefix_repeated = jnp.repeat(prefix_length, KEY_VALUE_HEADS, axis=0)
    loss_mask = (inside_document.reshape(TOKEN_TOTAL) >= prefix_length.reshape(TOKEN_TOTAL)).astype(jnp.float32)
    loss_count = jnp.sum(lengths - prefix_eff).astype(jnp.float32)
    onehot = (routes[:, :, None] == jnp.arange(EXPERTS, dtype=jnp.int32)[None, None, :]).astype(jnp.int32)
    chosen = lax.optimization_barrier(jnp.sum(onehot, axis=1)).astype(jnp.int32).reshape(blocks, TOK_DEV, EXPERTS)
    earlier = (jnp.cumsum(chosen, axis=1).astype(jnp.int32) - chosen).reshape(TOKEN_TOTAL, EXPERTS)
    slot_of = jnp.take_along_axis(earlier, routes, axis=1).astype(jnp.int32)
    block_of = (jnp.arange(TOKEN_TOTAL, dtype=jnp.int32) // TOK_DEV)[:, None]
    flat_index = (routes * (blocks * CAP) + block_of * CAP + slot_of).astype(jnp.int32)
    token_ids = jnp.broadcast_to(jnp.arange(TOKEN_TOTAL, dtype=jnp.int32)[:, None], flat_index.shape)
    source_row = jnp.zeros((EXPERTS * blocks * CAP,), jnp.int32).at[flat_index.reshape(-1)].set(token_ids.reshape(-1))
    filled = jnp.zeros((EXPERTS * blocks * CAP,), jnp.float32).at[flat_index.reshape(-1)].set(1.0)

    def forward(x_in, gain_first, wq_in, key_weight_input, value_weight_input, wo_in, gain_second, router_in, gate_in, up_in, down_in):
        inv_first = lax.rsqrt(lax.optimization_barrier(jnp.mean(x_in * x_in, axis=-1, keepdims=True)) + eps)
        first_activation = lower_precision(gain_first * (x_in * inv_first))
        query_matrix = lower_backward(matrix_product_exact(first_activation, wq_in)).reshape(TOKEN_TOTAL, QUERY_HEADS, HEAD_SIZE)
        key_matrix = lower_backward(matrix_product_exact(first_activation, key_weight_input)).reshape(TOKEN_TOTAL, KEY_VALUE_HEADS, HEAD_SIZE)
        value_matrix = lower_precision(lower_backward(matrix_product_exact(first_activation, value_weight_input))).reshape(TOKEN_TOTAL, KEY_VALUE_HEADS, HEAD_SIZE)
        query_matrix = lower_precision(rotate(query_matrix, cosine, sine_tab))
        key_matrix = lower_precision(rotate(key_matrix, cosine, sine_tab))
        query_grouped = query_matrix.reshape(PACK_COUNT, PACK_TOKENS, KEY_VALUE_HEADS, repeat_heads, HEAD_SIZE).transpose(0, 2, 1, 3, 4).reshape(PACK_COUNT * KEY_VALUE_HEADS, PACK_TOKENS, repeat_heads, HEAD_SIZE)
        key_grouped = key_matrix.reshape(PACK_COUNT, PACK_TOKENS, KEY_VALUE_HEADS, HEAD_SIZE).transpose(0, 2, 1, 3).reshape(PACK_COUNT * KEY_VALUE_HEADS, PACK_TOKENS, HEAD_SIZE)
        value_grouped = value_matrix.reshape(PACK_COUNT, PACK_TOKENS, KEY_VALUE_HEADS, HEAD_SIZE).transpose(0, 2, 1, 3).reshape(PACK_COUNT * KEY_VALUE_HEADS, PACK_TOKENS, HEAD_SIZE)
        attention_result = lax.map(jax.checkpoint(attend), (query_grouped, key_grouped, value_grouped, document_repeated, position_repeated, prefix_repeated))
        attention_result = attention_result.reshape(PACK_COUNT, KEY_VALUE_HEADS, PACK_TOKENS, repeat_heads, HEAD_SIZE).transpose(0, 2, 1, 3, 4).reshape(TOKEN_TOTAL, QUERY_HEADS * HEAD_SIZE)
        attention_result = lower_precision(lower_backward(attention_result))
        attn_out = lower_backward(matrix_product_exact(attention_result, wo_in))
        hidden_one = x_in + attn_out
        inv_second = lax.rsqrt(lax.optimization_barrier(jnp.mean(hidden_one * hidden_one, axis=-1, keepdims=True)) + eps)
        act_second = lower_precision(gain_second * (hidden_one * inv_second))
        logits = lower_backward(matrix_product_exact(act_second, router_in))
        chosen_logit = jnp.take_along_axis(logits, routes, axis=1)
        gate_probs = jax.nn.softmax(chosen_logit, axis=-1)
        routed = (act_second[source_row] * filled[:, None]).reshape(EXPERTS, blocks * CAP, MODEL_SIZE)
        expert_out = lax.map(jax.checkpoint(expert), (routed, gate_in, up_in, down_in))
        picked = expert_out.reshape(EXPERTS * blocks * CAP, MODEL_SIZE)[flat_index]
        moe_out = lax.optimization_barrier(jnp.sum(gate_probs[:, :, None] * picked, axis=1))
        return hidden_one + moe_out
    float_args = (tokens.astype(jnp.float32), attn_gain, wq.astype(jnp.float32), wk.astype(jnp.float32), wv.astype(jnp.float32), wo.astype(jnp.float32), moe_gain, router.astype(jnp.float32), w_gate.astype(jnp.float32), w_up.astype(jnp.float32), w_down.astype(jnp.float32))
    layer_out, pullback = jax.vjp(forward, *float_args)
    out_grad = loss_mask[:, None] * (layer_out - targets.astype(jnp.float32)) * (TOKEN_TOTAL / loss_count)
    gradients = pullback(out_grad)
    return (layer_out, gradients[0], gradients[1], gradients[2], gradients[3], gradients[4], gradients[5], gradients[6], gradients[7], gradients[8], gradients[9], gradients[10])
```

```python
import math

import jax
import jax.numpy as jnp
from jax import lax
from jax.sharding import PartitionSpec as P

HEAD_SIZE = 64
CAP = 32
GATHER_MAX = 8

eps = 1e-06
neg_big = -1e30
F32 = jnp.float32
BF16 = jnp.bfloat16


def dot_rows(first_mat, second_mat):
    return lax.dot_general(
        first_mat, second_mat, (((0,), (0,)), ((), ())), preferred_element_type=F32
    )


def dot_cols(first_mat, second_mat):
    return lax.dot_general(
        first_mat, second_mat, (((1,), (1,)), ((), ())), preferred_element_type=F32
    )


def rotate(tensor, cosine, sine_tab, direction):
    half_dim = tensor.shape[-1] // 2
    first_half = tensor[..., :half_dim]
    second_half = tensor[..., half_dim:]
    return jnp.concatenate(
        [
            first_half * cosine - direction * second_half * sine_tab,
            second_half * cosine + direction * first_half * sine_tab,
        ],
        axis=-1,
    )


def doc_layout(doc_lengths, prefix_lens, places):
    doc_ends = jnp.cumsum(doc_lengths)
    starts = doc_ends - doc_lengths
    document_index = jnp.sum((places[:, None] >= doc_ends[None, :]).astype(jnp.int32), axis=1)
    pick_doc = (
        document_index[:, None] == jnp.arange(doc_lengths.shape[0], dtype=jnp.int32)[None, :]
    ).astype(jnp.int32)
    inside_document = places - jnp.sum(pick_doc * starts[None, :], axis=1)
    prefix_length = jnp.sum(pick_doc * prefix_lens[None, :], axis=1)
    return (document_index, inside_document, prefix_length)


class Ring:
    def __init__(self, count):
        self.count = count
        self.order = list(range(0, count, 2)) + list(range(count - 1, 0, -2))
        here = lax.axis_index("seq")
        self.place = jnp.where(here % 2 == 0, here // 2, count - 1 - here // 2)

    def index_at(self, place):
        place = lax.rem(place + self.count, self.count)
        return jnp.where(
            place < self.count // 2, 2 * place, 2 * (self.count - 1 - place) + 1
        )

    def shift(self, value, step):
        pairs = [
            (self.order[i], self.order[(i + step) % self.count]) for i in range(self.count)
        ]
        return lax.ppermute(value, "seq", pairs)

    def gather(self, value):
        got = [None] * self.count
        got[0] = value
        right = left = value
        for step in range(1, self.count // 2 + 1):
            right = self.shift(right, 1)
            got[step] = right
            if step < self.count - step:
                left = self.shift(left, -1)
                got[self.count - step] = left
        return got

    def gather_one_way(self, value, step):
        got = [value]
        for i in range(1, self.count):
            got.append(self.shift(got[-1], step))
        return got if step == 1 else got[:1] + got[:0:-1]

    def scatter_sum(self, parts):
        half = self.count // 2
        total = parts[0].astype(F32)
        run = None
        for step in range(half, 0, -1):
            piece = parts[self.count - step].astype(F32)
            run = piece if run is None else piece + run.astype(F32)
            run = self.shift(run.astype(BF16), 1)
        back = None
        for step in range(half - 1, 0, -1):
            piece = parts[step].astype(F32)
            back = piece if back is None else piece + back.astype(F32)
            back = self.shift(back.astype(BF16), -1)
        total = total + run.astype(F32)
        return total if back is None else total + back.astype(F32)

    def in_order(self, got):
        turned = jnp.stack([got[0]] + got[:0:-1])
        twice = jnp.concatenate([turned, turned])
        start = lax.rem(self.count - self.place, self.count)
        return lax.dynamic_slice_in_dim(twice, start, self.count, axis=0)

    def exchange(self, pieces):
        got = []
        for step in range(self.count):
            mine = lax.dynamic_index_in_dim(
                pieces, self.index_at(self.place + step), axis=0, keepdims=False
            )
            got.append(mine if step == 0 else self.shift(mine, step))
        return got


def swap(value, axis):
    return lax.ppermute(value, axis, [(0, 1), (1, 0)])


def pair_sum(value):
    low = value.astype(BF16)
    return low.astype(F32) + swap(low, "tp").astype(F32)


def sum_all(value, seq_count):
    value = value + swap(value, "exp")
    step = 1
    while step < seq_count:
        value = value + lax.ppermute(value, "seq", [(i, i ^ step) for i in range(seq_count)])
        step *= 2
    return value


def slots_of(routes, experts):
    rows = routes.shape[-2]
    chosen = jnp.sum(
        (routes[..., None] == jnp.arange(experts, dtype=jnp.int32)).astype(F32), axis=-2
    )
    lower = jnp.tril(jnp.ones((rows, rows), BF16), -1)
    earlier = jnp.einsum(
        "st,...te->...se", lower, chosen.astype(BF16), preferred_element_type=F32
    )
    return chosen, earlier


def place_rows(chosen, earlier):
    slots = jnp.where(chosen > 0, earlier, -1.0).astype(jnp.int32)
    slots = jnp.swapaxes(slots, -1, -2)
    return (
        slots[..., :, None, :] == jnp.arange(CAP, dtype=jnp.int32)[:, None]
    ).astype(BF16)


def per_device(
    tokens,
    targets,
    attn_gain,
    wq,
    wk,
    wv,
    wo,
    moe_gain,
    router,
    w_gate,
    w_up,
    w_down,
    routes,
    lengths,
    prefix,
):
    rows_dev, model_width = tokens.shape
    exp_count = lax.axis_size("exp")
    seq_count = lax.axis_size("seq")
    exp_at = lax.axis_index("exp")
    seq_at = lax.axis_index("seq")
    ring = Ring(seq_count)
    pack_len = rows_dev * seq_count
    heads_q = wq.shape[1] // HEAD_SIZE
    heads_kv = wk.shape[1] // HEAD_SIZE
    kv_width = heads_kv * HEAD_SIZE
    repeat_heads = heads_q // heads_kv
    experts = router.shape[1]
    local_experts, _, units = w_gate.shape
    slice_width = model_width // seq_count
    scaling = 1.0 / math.sqrt(HEAD_SIZE)
    prefix_eff = jnp.minimum(prefix, lengths - 1)
    doc_lengths = lengths[exp_at]
    prefix_lens = prefix_eff[exp_at]
    block_at = ring.index_at(ring.place - jnp.arange(seq_count, dtype=jnp.int32))
    key_place = (
        block_at[:, None] * rows_dev + jnp.arange(rows_dev, dtype=jnp.int32)[None, :]
    ).reshape(pack_len)
    key_doc, key_local = doc_layout(doc_lengths, prefix_lens, key_place)[:2]
    query_place = seq_at * rows_dev + jnp.arange(rows_dev, dtype=jnp.int32)
    query_doc, query_local, query_limit = doc_layout(doc_lengths, prefix_lens, query_place)
    loss_count = jnp.sum(lengths - prefix_eff).astype(F32)
    factor = rows_dev * exp_count * seq_count / loss_count
    loss_mask = (query_local >= query_limit).astype(F32)
    frequency = jnp.exp(
        jnp.arange(HEAD_SIZE // 2, dtype=F32) * (-2.0 * math.log(10000.0) / HEAD_SIZE)
    )
    angles = query_local.astype(F32)[:, None, None] * frequency[None, None, :]
    cosine = jnp.cos(angles)
    sine_tab = jnp.sin(angles)

    x_full = tokens.astype(F32)
    inv_first = lax.rsqrt(jnp.mean(x_full * x_full, axis=1, keepdims=True) + eps)
    norm_first = x_full * inv_first
    first_activation = (attn_gain * norm_first).astype(BF16)
    key_matrix = jnp.dot(first_activation, wk, preferred_element_type=F32).reshape(
        rows_dev, heads_kv, HEAD_SIZE
    )
    key_matrix = rotate(key_matrix, cosine, sine_tab, 1.0).astype(BF16).reshape(rows_dev, kv_width)
    value_matrix = jnp.dot(first_activation, wv, preferred_element_type=F32).astype(BF16)
    both = jnp.concatenate(ring.gather(jnp.concatenate([key_matrix, value_matrix], axis=1)))
    query_matrix = jnp.dot(first_activation, wq, preferred_element_type=F32).reshape(
        rows_dev, heads_q, HEAD_SIZE
    )
    query_matrix = rotate(query_matrix, cosine, sine_tab, 1.0).astype(BF16)
    route_pair = jnp.stack([routes, swap(routes, "exp")])
    route_all = jnp.stack(ring.gather(route_pair))
    first_all = ring.in_order(ring.gather(first_activation))
    first_other = swap(first_all, "exp")

    key_all = both[:, :kv_width].reshape(pack_len, heads_kv, HEAD_SIZE)
    value_all = both[:, kv_width:].reshape(pack_len, heads_kv, HEAD_SIZE)
    query_heads = query_matrix.reshape(rows_dev, heads_kv, repeat_heads, HEAD_SIZE)
    allowed = (query_doc[:, None] == key_doc[None, :]) & (
        (key_place[None, :] <= query_place[:, None]) | (key_local[None, :] < query_limit[:, None])
    )
    scores = jnp.einsum("qgrd,kgd->grqk", query_heads, key_all, preferred_element_type=F32)
    scores = jnp.where(allowed, scores * scaling, neg_big)
    row_peak = jnp.max(scores, axis=-1, keepdims=True)
    probs = jnp.exp(scores - row_peak)
    probs = probs / jnp.sum(probs, axis=-1, keepdims=True)
    probs_low = probs.astype(BF16)
    attended_heads = jnp.einsum(
        "grqk,kgd->qgrd", probs_low, value_all, preferred_element_type=F32
    )
    attended_low = attended_heads.reshape(rows_dev, heads_q * HEAD_SIZE).astype(BF16)
    attn_out = pair_sum(jnp.dot(attended_low, wo, preferred_element_type=F32))
    attended_all = ring.in_order(ring.gather(attended_low))
    attended_other = swap(attended_all, "exp")

    hidden_one = x_full + attn_out
    inv_second = lax.rsqrt(jnp.mean(hidden_one * hidden_one, axis=1, keepdims=True) + eps)
    norm_second = hidden_one * inv_second
    act_second = (moe_gain * norm_second).astype(BF16)
    act_pair = jnp.stack([act_second, swap(act_second, "exp")])
    chosen_all, earlier_all = slots_of(route_all, experts)
    chosen_pair = chosen_all[0]
    logits = jnp.einsum("ptd,de->pte", act_pair, router, preferred_element_type=F32)
    logits = jnp.where(chosen_pair > 0, logits, neg_big)
    grown = jnp.where(
        chosen_pair > 0, jnp.exp(logits - jnp.max(logits, axis=-1, keepdims=True)), 0.0
    )
    gates = grown / jnp.sum(grown, axis=-1, keepdims=True)

    def own_experts(value):
        return lax.dynamic_slice_in_dim(value, exp_at * local_experts, local_experts, axis=-1)

    spots_all = place_rows(own_experts(chosen_all), own_experts(earlier_all))
    spots = spots_all[0]
    row_gate = jnp.einsum(
        "pect,pte->epc", spots.astype(F32), own_experts(gates), precision=lax.Precision.HIGHEST
    ).reshape(local_experts, exp_count * CAP, 1)

    def to_rows(value):
        rows = jnp.einsum("pect,ptd->epcd", spots, value, preferred_element_type=F32)
        return rows.astype(BF16).reshape(local_experts, exp_count * CAP, model_width)

    def to_tokens(rows):
        rows = rows.reshape(local_experts, exp_count, CAP, model_width)
        part = jnp.einsum("pect,epcd->ptd", spots, rows, preferred_element_type=F32)
        return part

    arrived = to_rows(act_pair)
    gate_pre = jnp.einsum("ecd,edf->ecf", arrived, w_gate, preferred_element_type=F32)
    up_pre = jnp.einsum("ecd,edf->ecf", arrived, w_up, preferred_element_type=F32)
    sigma_gate = jax.nn.sigmoid(gate_pre)
    swish_gate = gate_pre * sigma_gate
    inner_act = (swish_gate * up_pre).astype(BF16)
    gated_act = (row_gate * inner_act.astype(F32)).astype(BF16)
    half = local_experts // 2
    gather_expert_rows = seq_count <= GATHER_MAX
    if gather_expert_rows:
        hid_right = ring.gather_one_way(gated_act[:half], 1)
        hid_left = ring.gather_one_way(gated_act[half:], -1)
    partial_out = jnp.einsum(
        "ecf,efd->ecd", inner_act, w_down, preferred_element_type=F32
    ).astype(BF16)
    moe_part = to_tokens((row_gate * partial_out.astype(F32)).astype(BF16))
    moe_part = moe_part[0] + swap(moe_part[1].astype(BF16), "exp").astype(F32)
    moe_out = pair_sum(moe_part)
    layer_out = hidden_one + moe_out

    out_grad = loss_mask[:, None] * (layer_out - targets.astype(F32)) * factor
    out_low = out_grad.astype(BF16)
    out_pair = jnp.stack([out_low, swap(out_low, "exp")])
    grad_rows = to_rows(out_pair)
    inner_grad = jnp.einsum("ecd,efd->ecf", grad_rows, w_down, preferred_element_type=F32)
    row_sens = jnp.sum(inner_act.astype(F32) * inner_grad, axis=-1)
    inner_grad = inner_grad * row_gate
    gate_rows = (inner_grad * up_pre * sigma_gate * (1.0 + gate_pre * (1.0 - sigma_gate))).astype(
        BF16
    )
    up_rows = (inner_grad * swish_gate).astype(BF16)
    gate_up = jnp.concatenate([gate_rows, up_rows], axis=-1)
    back_rows = jnp.einsum("ecf,edf->ecd", gate_rows, w_gate, preferred_element_type=F32)
    back_rows = (
        back_rows + jnp.einsum("ecf,edf->ecd", up_rows, w_up, preferred_element_type=F32)
    ).astype(BF16)
    back_part = to_tokens(back_rows)
    sens_part = jnp.einsum(
        "pect,epc->pte",
        spots.astype(F32),
        row_sens.reshape(local_experts, exp_count, CAP),
        precision=lax.Precision.HIGHEST,
    )
    sens_part = lax.dynamic_update_slice_in_dim(
        jnp.zeros((exp_count, rows_dev, 128), F32), sens_part, exp_at * local_experts, axis=2
    )
    back_part = jnp.concatenate([back_part, sens_part], axis=2)
    back_part = back_part[0] + swap(back_part[1].astype(BF16), "exp").astype(F32)
    back_sum = pair_sum(back_part)
    moe_in_grad = back_sum[:, :model_width]
    gate_sens = back_sum[:, model_width : model_width + experts]
    own_gates = gates[0]
    centered = own_gates * (gate_sens - jnp.sum(own_gates * gate_sens, axis=1, keepdims=True))
    logit_grad = centered.astype(BF16)
    router_wgrad = dot_rows(logit_grad, act_second)
    act_second_grad = moe_in_grad + dot_cols(logit_grad, router)
    scaled_second = moe_gain * act_second_grad
    hidden_grad = out_grad + inv_second * (
        scaled_second - norm_second * jnp.mean(scaled_second * norm_second, axis=1, keepdims=True)
    )
    moe_gain_grad = jnp.sum(act_second_grad * norm_second, axis=0)
    small_sum = sum_all(jnp.concatenate([router_wgrad, moe_gain_grad[None]]), seq_count)
    hidden_low = hidden_grad.astype(BF16)

    grad_heads = (
        dot_cols(hidden_low, wo)
        .astype(BF16)
        .reshape(rows_dev, heads_kv, repeat_heads, HEAD_SIZE)
    )
    delta_rows = jnp.transpose(
        jnp.sum(grad_heads.astype(F32) * attended_heads, axis=-1), (1, 2, 0)
    )
    prob_grad = jnp.einsum("qgrd,kgd->grqk", grad_heads, value_all, preferred_element_type=F32)
    score_grad = (probs * (prob_grad - delta_rows[..., None])).astype(BF16)
    query_grad = jnp.einsum("grqk,kgd->qgrd", score_grad, key_all, preferred_element_type=F32)
    key_parts = (
        jnp.einsum("grqk,qgrd->kgd", score_grad, query_heads, preferred_element_type=F32) * scaling
    )
    value_parts = jnp.einsum("grqk,qgrd->kgd", probs_low, grad_heads, preferred_element_type=F32)
    both_parts = jnp.concatenate(
        [
            key_parts.reshape(seq_count, rows_dev, kv_width),
            value_parts.reshape(seq_count, rows_dev, kv_width),
        ],
        axis=2,
    ).astype(BF16)
    both_sum = ring.scatter_sum([both_parts[i] for i in range(seq_count)])
    query_grad = (
        rotate(query_grad.reshape(rows_dev, heads_q, HEAD_SIZE) * scaling, cosine, sine_tab, -1.0)
        .astype(BF16)
        .reshape(rows_dev, heads_q * HEAD_SIZE)
    )
    key_grad = (
        rotate(
            both_sum[:, :kv_width].reshape(rows_dev, heads_kv, HEAD_SIZE), cosine, sine_tab, -1.0
        )
        .astype(BF16)
        .reshape(rows_dev, kv_width)
    )
    value_grad = both_sum[:, kv_width:].astype(BF16)
    first_part = dot_cols(query_grad, wq) + dot_cols(key_grad, wk) + dot_cols(value_grad, wv)
    act_first_grad = pair_sum(first_part)
    scaled_first = attn_gain * act_first_grad
    input_grad = hidden_grad + inv_first * (
        scaled_first - norm_first * jnp.mean(scaled_first * norm_first, axis=1, keepdims=True)
    )
    attn_gain_grad = sum_all(jnp.sum(act_first_grad * norm_first, axis=0), seq_count)

    def over_tokens(first_own, first_oth, second_own, second_oth):
        def flat(value):
            return value.reshape(pack_len, value.shape[-1])

        return dot_rows(flat(first_own), flat(second_own)) + dot_rows(
            flat(first_oth), flat(second_oth)
        )

    hidden_all = ring.in_order(ring.gather(hidden_low))
    wo_wgrad = over_tokens(attended_all, attended_other, hidden_all, swap(hidden_all, "exp"))
    query_all = ring.in_order(ring.gather(query_grad))
    wq_wgrad = over_tokens(first_all, first_other, query_all, swap(query_all, "exp"))
    pair_all = ring.in_order(ring.gather(jnp.concatenate([key_grad, value_grad], axis=1)))
    wkv_wgrad = over_tokens(first_all, first_other, pair_all, swap(pair_all, "exp"))

    if gather_expert_rows:

        def column_slices(value):
            pieces = jnp.transpose(value.reshape(rows_dev, seq_count, slice_width), (1, 0, 2))
            own = jnp.stack(ring.exchange(pieces))
            return jnp.stack([own, swap(own, "exp")], axis=1)

        def rows_of_all(slices):
            rows = jnp.einsum("kpect,kptd->ekpcd", spots_all, slices, preferred_element_type=F32)
            return rows.astype(BF16).reshape(local_experts, seq_count * exp_count * CAP, slice_width)

        act_rows = rows_of_all(column_slices(act_second))
        out_rows = rows_of_all(column_slices(out_low))
        pre_right = ring.gather_one_way(gate_up[:half], 1)
        pre_left = ring.gather_one_way(gate_up[half:], -1)

        def expert_wgrads(hid, pre, act, out):
            hid = jnp.concatenate(hid, axis=1)
            pre = jnp.concatenate(pre, axis=1)
            down = jnp.einsum("ecf,ecd->efd", hid, out, preferred_element_type=F32)
            gate = jnp.einsum("ecd,ecf->edf", act, pre[..., :units], preferred_element_type=F32)
            up = jnp.einsum("ecd,ecf->edf", act, pre[..., units:], preferred_element_type=F32)
            return gate, up, down

        first_grads = expert_wgrads(hid_right, pre_right, act_rows[:half], out_rows[:half])
        second_grads = expert_wgrads(hid_left, pre_left, act_rows[half:], out_rows[half:])
        expert_sums = [jnp.concatenate(pair) for pair in zip(first_grads, second_grads)]
    else:

        def scattered(first, second, dim):
            grad = jnp.einsum("ecd,ecf->edf", first, second, preferred_element_type=F32)
            return lax.psum_scatter(
                grad.astype(BF16), "seq", scatter_dimension=dim, tiled=True
            ).astype(F32)

        expert_sums = [
            scattered(arrived, gate_rows, 1),
            scattered(arrived, up_rows, 1),
            scattered(gated_act, grad_rows, 2),
        ]
    return (
        layer_out,
        input_grad,
        attn_gain_grad,
        wq_wgrad,
        wkv_wgrad[:, :kv_width],
        wkv_wgrad[:, kv_width:],
        wo_wgrad,
        small_sum[experts],
        small_sum[:experts].T,
        expert_sums[0],
        expert_sums[1],
        expert_sums[2],
    )


def solution(mesh):
    return jax.shard_map(
        per_device,
        mesh=mesh,
        in_specs=(
            P(("exp", "seq"), None),
            P(("exp", "seq"), None),
            P(),
            P(None, "tp"),
            P(None, "tp"),
            P(None, "tp"),
            P("tp", None),
            P(),
            P(),
            P("exp", None, "tp"),
            P("exp", None, "tp"),
            P("exp", "tp", None),
            P(("exp", "seq"), None),
            P(),
            P(),
        ),
        out_specs=(
            P(("exp", "seq"), None),
            P(("exp", "seq"), None),
            P(),
            P(None, "tp"),
            P(None, "tp"),
            P(None, "tp"),
            P("tp", None),
            P(),
            P(),
            P("exp", "seq", "tp"),
            P("exp", "seq", "tp"),
            P("exp", "tp", "seq"),
        ),
        check_vma=False,
    )
```

```python
import math

import jax
import jax.numpy as jnp
from jax import lax
from jax.experimental import pallas as pl
from jax.sharding import PartitionSpec as P

HEAD_SIZE = 64
CAP = 32
GATHER_MAX = 8

eps = 1e-06
neg_big = -1e30
F32 = jnp.float32
BF16 = jnp.bfloat16


def dot_rows(first_mat, second_mat):
    return lax.dot_general(
        first_mat, second_mat, (((0,), (0,)), ((), ())), preferred_element_type=F32
    )


def dot_cols(first_mat, second_mat):
    return lax.dot_general(
        first_mat, second_mat, (((1,), (1,)), ((), ())), preferred_element_type=F32
    )


def rotate(tensor, cosine, sine_tab, direction):
    half_dim = tensor.shape[-1] // 2
    first_half = tensor[..., :half_dim]
    second_half = tensor[..., half_dim:]
    return jnp.concatenate(
        [
            first_half * cosine - direction * second_half * sine_tab,
            second_half * cosine + direction * first_half * sine_tab,
        ],
        axis=-1,
    )


def doc_layout(doc_lengths, prefix_lens, places):
    doc_ends = jnp.cumsum(doc_lengths)
    starts = doc_ends - doc_lengths
    document_index = jnp.sum((places[:, None] >= doc_ends[None, :]).astype(jnp.int32), axis=1)
    pick_doc = (
        document_index[:, None] == jnp.arange(doc_lengths.shape[0], dtype=jnp.int32)[None, :]
    ).astype(jnp.int32)
    inside_document = places - jnp.sum(pick_doc * starts[None, :], axis=1)
    prefix_length = jnp.sum(pick_doc * prefix_lens[None, :], axis=1)
    return (document_index, inside_document, prefix_length)


class Ring:
    def __init__(self, count):
        self.count = count
        self.order = list(range(0, count, 2)) + list(range(count - 1, 0, -2))
        here = lax.axis_index("seq")
        self.place = jnp.where(here % 2 == 0, here // 2, count - 1 - here // 2)

    def index_at(self, place):
        place = lax.rem(place + self.count, self.count)
        return jnp.where(
            place < self.count // 2, 2 * place, 2 * (self.count - 1 - place) + 1
        )

    def shift(self, value, step):
        pairs = [
            (self.order[i], self.order[(i + step) % self.count]) for i in range(self.count)
        ]
        return lax.ppermute(value, "seq", pairs)

    def gather(self, value):
        got = [None] * self.count
        got[0] = value
        right = left = value
        for step in range(1, self.count // 2 + 1):
            right = self.shift(right, 1)
            got[step] = right
            if step < self.count - step:
                left = self.shift(left, -1)
                got[self.count - step] = left
        return got

    def scatter_sum(self, parts):
        half = self.count // 2
        total = parts[0].astype(F32)
        run = None
        for step in range(half, 0, -1):
            piece = parts[self.count - step].astype(F32)
            run = piece if run is None else piece + run.astype(F32)
            run = self.shift(run.astype(BF16), 1)
        back = None
        for step in range(half - 1, 0, -1):
            piece = parts[step].astype(F32)
            back = piece if back is None else piece + back.astype(F32)
            back = self.shift(back.astype(BF16), -1)
        total = total + run.astype(F32)
        return total if back is None else total + back.astype(F32)

    def in_order(self, got):
        filled = jnp.zeros((self.count,) + got[0].shape, got[0].dtype)
        for step, piece in enumerate(got):
            place = lax.rem(self.place - step + self.count, self.count)
            filled = lax.dynamic_update_index_in_dim(filled, piece, place, axis=0)
        return filled

    def exchange(self, pieces):
        got = []
        for step in range(self.count):
            mine = lax.dynamic_index_in_dim(
                pieces, self.index_at(self.place + step), axis=0, keepdims=False
            )
            got.append(mine if step == 0 else self.shift(mine, step))
        return got


def swap(value, axis):
    return lax.ppermute(value, axis, [(0, 1), (1, 0)])


def pair_sum(value):
    low = value.astype(BF16)
    return low.astype(F32) + swap(low, "tp").astype(F32)


def sum_all(value, seq_count):
    value = value + swap(value, "exp")
    step = 1
    while step < seq_count:
        value = value + lax.ppermute(value, "seq", [(i, i ^ step) for i in range(seq_count)])
        step *= 2
    return value


def slots_of(routes, experts):
    rows = routes.shape[-2]
    chosen = jnp.sum(
        (routes[..., None] == jnp.arange(experts, dtype=jnp.int32)).astype(F32), axis=-2
    )
    lower = jnp.tril(jnp.ones((rows, rows), BF16), -1)
    earlier = jnp.einsum(
        "st,...te->...se", lower, chosen.astype(BF16), preferred_element_type=F32
    )
    return chosen, earlier


def place_rows(chosen, earlier):
    slots = jnp.where(chosen > 0, earlier, -1.0).astype(jnp.int32)
    slots = jnp.swapaxes(slots, -1, -2)
    return (
        slots[..., :, None, :] == jnp.arange(CAP, dtype=jnp.int32)[:, None]
    ).astype(BF16)


def wgrad_kernel(count, *refs):
    hid_refs, pre_refs = refs[:count], refs[count : 2 * count]
    act_ref, out_ref, gate_ref, up_ref, down_ref = refs[2 * count :]
    hid = jnp.concatenate([ref[0] for ref in hid_refs], axis=0)
    pre = jnp.concatenate([ref[0] for ref in pre_refs], axis=0)
    units = hid.shape[1]
    width = act_ref.shape[-1]
    act = act_ref[...].reshape(hid.shape[0], width)
    out = out_ref[...].reshape(hid.shape[0], width)
    both = dot_rows(act, pre)
    gate_ref[0] = both[:, :units]
    up_ref[0] = both[:, units:]
    down_ref[0] = dot_rows(hid, out)


def expert_wgrads(hid, pre, act, out):
    count = len(hid)
    local_experts, rows, units = hid[0].shape
    seq_count, packs, _, cap, width = act.shape

    def by_expert(height, columns):
        return pl.BlockSpec((1, height, columns), lambda e: (e, 0, 0))

    rows_spec = pl.BlockSpec((seq_count, packs, 1, cap, width), lambda e: (0, 0, e, 0, 0))
    return pl.pallas_call(
        lambda *refs: wgrad_kernel(count, *refs),
        grid=(local_experts,),
        in_specs=[by_expert(rows, units)] * count
        + [by_expert(rows, 2 * units)] * count
        + [rows_spec] * 2,
        out_specs=[by_expert(width, units)] * 2 + [by_expert(units, width)],
        out_shape=[jax.ShapeDtypeStruct((local_experts, width, units), F32)] * 2
        + [jax.ShapeDtypeStruct((local_experts, units, width), F32)],
        cost_estimate=pl.CostEstimate(
            flops=6 * local_experts * count * rows * units * width,
            bytes_accessed=40_000_000,
            transcendentals=0,
        ),
        name="expert_wgrads",
    )(*hid, *pre, act, out)


def per_device(
    tokens,
    targets,
    attn_gain,
    wq,
    wk,
    wv,
    wo,
    moe_gain,
    router,
    w_gate,
    w_up,
    w_down,
    routes,
    lengths,
    prefix,
):
    rows_dev, model_width = tokens.shape
    exp_count = lax.axis_size("exp")
    seq_count = lax.axis_size("seq")
    exp_at = lax.axis_index("exp")
    seq_at = lax.axis_index("seq")
    ring = Ring(seq_count)
    pack_len = rows_dev * seq_count
    heads_q = wq.shape[1] // HEAD_SIZE
    heads_kv = wk.shape[1] // HEAD_SIZE
    kv_width = heads_kv * HEAD_SIZE
    repeat_heads = heads_q // heads_kv
    experts = router.shape[1]
    local_experts, _, units = w_gate.shape
    slice_width = model_width // seq_count
    scaling = 1.0 / math.sqrt(HEAD_SIZE)
    prefix_eff = jnp.minimum(prefix, lengths - 1)
    doc_lengths = lengths[exp_at]
    prefix_lens = prefix_eff[exp_at]
    block_at = ring.index_at(ring.place - jnp.arange(seq_count, dtype=jnp.int32))
    key_place = (
        block_at[:, None] * rows_dev + jnp.arange(rows_dev, dtype=jnp.int32)[None, :]
    ).reshape(pack_len)
    key_doc, key_local = doc_layout(doc_lengths, prefix_lens, key_place)[:2]
    query_place = seq_at * rows_dev + jnp.arange(rows_dev, dtype=jnp.int32)
    query_doc, query_local, query_limit = doc_layout(doc_lengths, prefix_lens, query_place)
    loss_count = jnp.sum(lengths - prefix_eff).astype(F32)
    factor = rows_dev * exp_count * seq_count / loss_count
    loss_mask = (query_local >= query_limit).astype(F32)
    frequency = jnp.exp(
        jnp.arange(HEAD_SIZE // 2, dtype=F32) * (-2.0 * math.log(10000.0) / HEAD_SIZE)
    )
    angles = query_local.astype(F32)[:, None, None] * frequency[None, None, :]
    cosine = jnp.cos(angles)
    sine_tab = jnp.sin(angles)

    x_full = tokens.astype(F32)
    inv_first = lax.rsqrt(jnp.mean(x_full * x_full, axis=1, keepdims=True) + eps)
    norm_first = x_full * inv_first
    first_activation = (attn_gain * norm_first).astype(BF16)
    key_matrix = jnp.dot(first_activation, wk, preferred_element_type=F32).reshape(
        rows_dev, heads_kv, HEAD_SIZE
    )
    key_matrix = rotate(key_matrix, cosine, sine_tab, 1.0).astype(BF16).reshape(rows_dev, kv_width)
    value_matrix = jnp.dot(first_activation, wv, preferred_element_type=F32).astype(BF16)
    both = jnp.concatenate(ring.gather(jnp.concatenate([key_matrix, value_matrix], axis=1)))
    query_matrix = jnp.dot(first_activation, wq, preferred_element_type=F32).reshape(
        rows_dev, heads_q, HEAD_SIZE
    )
    query_matrix = rotate(query_matrix, cosine, sine_tab, 1.0).astype(BF16)
    route_pair = jnp.concatenate([routes, swap(routes, "exp")], axis=1).astype(BF16)
    route_pad = 128 - route_pair.shape[1]
    first_got = ring.gather(
        jnp.concatenate([first_activation, jnp.pad(route_pair, ((0, 0), (0, route_pad)))], axis=1)
    )
    route_all = jnp.stack([got[:, model_width:] for got in first_got])
    route_all = route_all[..., : exp_count * routes.shape[1]].astype(jnp.int32)
    route_all = jnp.swapaxes(
        route_all.reshape(seq_count, rows_dev, exp_count, routes.shape[1]), 1, 2
    )
    first_all = ring.in_order([got[:, :model_width] for got in first_got])
    first_other = swap(first_all, "exp")

    key_all = both[:, :kv_width].reshape(pack_len, heads_kv, HEAD_SIZE)
    value_all = both[:, kv_width:].reshape(pack_len, heads_kv, HEAD_SIZE)
    query_heads = query_matrix.reshape(rows_dev, heads_kv, repeat_heads, HEAD_SIZE)
    allowed = (query_doc[:, None] == key_doc[None, :]) & (
        (key_place[None, :] <= query_place[:, None]) | (key_local[None, :] < query_limit[:, None])
    )
    scores = jnp.einsum("qgrd,kgd->grqk", query_heads, key_all, preferred_element_type=F32)
    scores = jnp.where(allowed, scores * scaling, neg_big)
    row_peak = jnp.max(scores, axis=-1, keepdims=True)
    probs = jnp.exp(scores - row_peak)
    probs = probs / jnp.sum(probs, axis=-1, keepdims=True)
    probs_low = probs.astype(BF16)
    attended_heads = jnp.einsum(
        "grqk,kgd->qgrd", probs_low, value_all, preferred_element_type=F32
    )
    attended_low = attended_heads.reshape(rows_dev, heads_q * HEAD_SIZE).astype(BF16)
    attn_out = pair_sum(jnp.dot(attended_low, wo, preferred_element_type=F32))

    hidden_one = x_full + attn_out
    inv_second = lax.rsqrt(jnp.mean(hidden_one * hidden_one, axis=1, keepdims=True) + eps)
    norm_second = hidden_one * inv_second
    act_second = (moe_gain * norm_second).astype(BF16)
    act_pair = jnp.stack([act_second, swap(act_second, "exp")])
    chosen_all, earlier_all = slots_of(route_all, experts)
    chosen_pair = chosen_all[0]
    logits = jnp.einsum("ptd,de->pte", act_pair, router, preferred_element_type=F32)
    logits = jnp.where(chosen_pair > 0, logits, neg_big)
    grown = jnp.where(
        chosen_pair > 0, jnp.exp(logits - jnp.max(logits, axis=-1, keepdims=True)), 0.0
    )
    gates = grown / jnp.sum(grown, axis=-1, keepdims=True)

    def own_experts(value):
        return lax.dynamic_slice_in_dim(value, exp_at * local_experts, local_experts, axis=-1)

    spots_all = place_rows(own_experts(chosen_all), own_experts(earlier_all))
    spots = spots_all[0]
    row_gate = jnp.einsum(
        "pect,pte->epc", spots.astype(F32), own_experts(gates), precision=lax.Precision.HIGHEST
    ).reshape(local_experts, exp_count * CAP, 1)

    def to_rows(value):
        rows = jnp.einsum("pect,ptd->epcd", spots, value, preferred_element_type=F32)
        return rows.astype(BF16).reshape(local_experts, exp_count * CAP, model_width)

    def to_tokens(rows):
        rows = rows.reshape(local_experts, exp_count, CAP, model_width)
        part = jnp.einsum("pect,epcd->ptd", spots, rows, preferred_element_type=F32)
        return part

    arrived = to_rows(act_pair)
    gate_pre = jnp.einsum("ecd,edf->ecf", arrived, w_gate, preferred_element_type=F32)
    up_pre = jnp.einsum("ecd,edf->ecf", arrived, w_up, preferred_element_type=F32)
    sigma_gate = jax.nn.sigmoid(gate_pre)
    swish_gate = gate_pre * sigma_gate
    inner_act = (swish_gate * up_pre).astype(BF16)
    gated_act = (row_gate * inner_act.astype(F32)).astype(BF16)
    gather_expert_rows = seq_count <= GATHER_MAX
    if gather_expert_rows:
        hid_got = ring.gather(gated_act)
    partial_out = jnp.einsum(
        "ecf,efd->ecd", inner_act, w_down, preferred_element_type=F32
    ).astype(BF16)
    moe_part = to_tokens((row_gate * partial_out.astype(F32)).astype(BF16))
    moe_part = moe_part[0] + swap(moe_part[1].astype(BF16), "exp").astype(F32)
    moe_out = pair_sum(moe_part)
    layer_out = hidden_one + moe_out

    out_grad = loss_mask[:, None] * (layer_out - targets.astype(F32)) * factor
    out_low = out_grad.astype(BF16)
    out_pair = jnp.stack([out_low, swap(out_low, "exp")])
    grad_rows = to_rows(out_pair)
    inner_grad = jnp.einsum("ecd,efd->ecf", grad_rows, w_down, preferred_element_type=F32)
    row_sens = jnp.sum(inner_act.astype(F32) * inner_grad, axis=-1)
    inner_grad = inner_grad * row_gate
    gate_rows = (inner_grad * up_pre * sigma_gate * (1.0 + gate_pre * (1.0 - sigma_gate))).astype(
        BF16
    )
    up_rows = (inner_grad * swish_gate).astype(BF16)
    gate_up = jnp.concatenate([gate_rows, up_rows], axis=-1)
    back_rows = jnp.einsum("ecf,edf->ecd", gate_rows, w_gate, preferred_element_type=F32)
    back_rows = (
        back_rows + jnp.einsum("ecf,edf->ecd", up_rows, w_up, preferred_element_type=F32)
    ).astype(BF16)
    back_part = to_tokens(back_rows)
    sens_part = jnp.einsum(
        "pect,epc->pte",
        spots.astype(F32),
        row_sens.reshape(local_experts, exp_count, CAP),
        precision=lax.Precision.HIGHEST,
    )
    sens_part = lax.dynamic_update_slice_in_dim(
        jnp.zeros((exp_count, rows_dev, 128), F32), sens_part, exp_at * local_experts, axis=2
    )
    back_part = jnp.concatenate([back_part, sens_part], axis=2)
    back_part = back_part[0] + swap(back_part[1].astype(BF16), "exp").astype(F32)
    back_sum = pair_sum(back_part)
    moe_in_grad = back_sum[:, :model_width]
    gate_sens = back_sum[:, model_width : model_width + experts]
    own_gates = gates[0]
    centered = own_gates * (gate_sens - jnp.sum(own_gates * gate_sens, axis=1, keepdims=True))
    logit_grad = centered.astype(BF16)
    router_wgrad = dot_rows(logit_grad, act_second)
    act_second_grad = moe_in_grad + dot_cols(logit_grad, router)
    scaled_second = moe_gain * act_second_grad
    hidden_grad = out_grad + inv_second * (
        scaled_second - norm_second * jnp.mean(scaled_second * norm_second, axis=1, keepdims=True)
    )
    moe_gain_grad = jnp.sum(act_second_grad * norm_second, axis=0)
    small_sum = sum_all(jnp.concatenate([router_wgrad, moe_gain_grad[None]]), seq_count)
    hidden_low = hidden_grad.astype(BF16)

    grad_heads = (
        dot_cols(hidden_low, wo)
        .astype(BF16)
        .reshape(rows_dev, heads_kv, repeat_heads, HEAD_SIZE)
    )
    delta_rows = jnp.transpose(
        jnp.sum(grad_heads.astype(F32) * attended_heads, axis=-1), (1, 2, 0)
    )
    prob_grad = jnp.einsum("qgrd,kgd->grqk", grad_heads, value_all, preferred_element_type=F32)
    score_grad = (probs * (prob_grad - delta_rows[..., None])).astype(BF16)
    query_grad = jnp.einsum("grqk,kgd->qgrd", score_grad, key_all, preferred_element_type=F32)
    key_parts = (
        jnp.einsum("grqk,qgrd->kgd", score_grad, query_heads, preferred_element_type=F32) * scaling
    )
    value_parts = jnp.einsum("grqk,qgrd->kgd", probs_low, grad_heads, preferred_element_type=F32)
    both_parts = jnp.concatenate(
        [
            key_parts.reshape(seq_count, rows_dev, kv_width),
            value_parts.reshape(seq_count, rows_dev, kv_width),
        ],
        axis=2,
    ).astype(BF16)
    both_sum = ring.scatter_sum([both_parts[i] for i in range(seq_count)])
    query_grad = (
        rotate(query_grad.reshape(rows_dev, heads_q, HEAD_SIZE) * scaling, cosine, sine_tab, -1.0)
        .astype(BF16)
        .reshape(rows_dev, heads_q * HEAD_SIZE)
    )
    key_grad = (
        rotate(
            both_sum[:, :kv_width].reshape(rows_dev, heads_kv, HEAD_SIZE), cosine, sine_tab, -1.0
        )
        .astype(BF16)
        .reshape(rows_dev, kv_width)
    )
    value_grad = both_sum[:, kv_width:].astype(BF16)
    first_part = dot_cols(query_grad, wq) + dot_cols(key_grad, wk) + dot_cols(value_grad, wv)
    act_first_grad = pair_sum(first_part)
    scaled_first = attn_gain * act_first_grad
    input_grad = hidden_grad + inv_first * (
        scaled_first - norm_first * jnp.mean(scaled_first * norm_first, axis=1, keepdims=True)
    )
    attn_gain_grad = sum_all(jnp.sum(act_first_grad * norm_first, axis=0), seq_count)

    def over_tokens(first_own, first_oth, second_own, second_oth):
        def flat(value):
            return value.reshape(pack_len, value.shape[-1])

        return dot_rows(flat(first_own), flat(second_own)) + dot_rows(
            flat(first_oth), flat(second_oth)
        )

    query_width = heads_q * HEAD_SIZE
    hidden_all = ring.in_order(ring.gather(jnp.concatenate([attended_low, hidden_low], axis=1)))
    hidden_other = swap(hidden_all, "exp")
    wo_wgrad = over_tokens(
        hidden_all[..., :query_width],
        hidden_other[..., :query_width],
        hidden_all[..., query_width:],
        hidden_other[..., query_width:],
    )
    grads_all = ring.in_order(
        ring.gather(jnp.concatenate([query_grad, key_grad, value_grad], axis=1))
    )
    grads_other = swap(grads_all, "exp")
    wq_wgrad = over_tokens(
        first_all, first_other, grads_all[..., :query_width], grads_other[..., :query_width]
    )
    wkv_wgrad = over_tokens(
        first_all, first_other, grads_all[..., query_width:], grads_other[..., query_width:]
    )

    if gather_expert_rows:

        def pieces_of(value):
            return jnp.transpose(value.reshape(rows_dev, seq_count, slice_width), (1, 0, 2))

        slices = jnp.stack(
            ring.exchange(jnp.concatenate([pieces_of(act_second), pieces_of(out_low)], axis=2))
        )
        slices = jnp.stack([slices, swap(slices, "exp")], axis=1)

        def rows_of_all(value):
            rows = jnp.einsum("kpect,kptd->kpecd", spots_all, value, preferred_element_type=F32)
            return rows.astype(BF16)

        expert_sums = expert_wgrads(
            hid_got,
            ring.gather(gate_up),
            rows_of_all(slices[..., :slice_width]),
            rows_of_all(slices[..., slice_width:]),
        )
    else:

        def scattered(first, second, dim):
            grad = jnp.einsum("ecd,ecf->edf", first, second, preferred_element_type=F32)
            return lax.psum_scatter(
                grad.astype(BF16), "seq", scatter_dimension=dim, tiled=True
            ).astype(F32)

        expert_sums = [
            scattered(arrived, gate_rows, 1),
            scattered(arrived, up_rows, 1),
            scattered(gated_act, grad_rows, 2),
        ]
    return (
        layer_out,
        input_grad,
        attn_gain_grad,
        wq_wgrad,
        wkv_wgrad[:, :kv_width],
        wkv_wgrad[:, kv_width:],
        wo_wgrad,
        small_sum[experts],
        small_sum[:experts].T,
        expert_sums[0],
        expert_sums[1],
        expert_sums[2],
    )


def solution(mesh):
    return jax.shard_map(
        per_device,
        mesh=mesh,
        in_specs=(
            P(("exp", "seq"), None),
            P(("exp", "seq"), None),
            P(),
            P(None, "tp"),
            P(None, "tp"),
            P(None, "tp"),
            P("tp", None),
            P(),
            P(),
            P("exp", None, "tp"),
            P("exp", None, "tp"),
            P("exp", "tp", None),
            P(("exp", "seq"), None),
            P(),
            P(),
        ),
        out_specs=(
            P(("exp", "seq"), None),
            P(("exp", "seq"), None),
            P(),
            P(None, "tp"),
            P(None, "tp"),
            P(None, "tp"),
            P("tp", None),
            P(),
            P(),
            P("exp", "seq", "tp"),
            P("exp", "seq", "tp"),
            P("exp", "tp", "seq"),
        ),
        check_vma=False,
    )
```

```python
import math

import jax
import jax.numpy as jnp
from jax import lax
from jax.experimental import pallas as pl
from jax.sharding import PartitionSpec as P

HEAD_SIZE = 64
CAP = 32
GATHER_MAX = 8

eps = 1e-06
neg_big = -1e30
F32 = jnp.float32
BF16 = jnp.bfloat16


def dot_rows(first_mat, second_mat):
    return lax.dot_general(
        first_mat, second_mat, (((0,), (0,)), ((), ())), preferred_element_type=F32
    )


def dot_cols(first_mat, second_mat):
    return lax.dot_general(
        first_mat, second_mat, (((1,), (1,)), ((), ())), preferred_element_type=F32
    )


def rotate(tensor, cosine, sine_tab, direction):
    half_dim = tensor.shape[-1] // 2
    first_half = tensor[..., :half_dim]
    second_half = tensor[..., half_dim:]
    return jnp.concatenate(
        [
            first_half * cosine - direction * second_half * sine_tab,
            second_half * cosine + direction * first_half * sine_tab,
        ],
        axis=-1,
    )


def doc_layout(doc_lengths, prefix_lens, places):
    doc_ends = jnp.cumsum(doc_lengths)
    starts = doc_ends - doc_lengths
    document_index = jnp.sum((places[:, None] >= doc_ends[None, :]).astype(jnp.int32), axis=1)
    pick_doc = (
        document_index[:, None] == jnp.arange(doc_lengths.shape[0], dtype=jnp.int32)[None, :]
    ).astype(jnp.int32)
    inside_document = places - jnp.sum(pick_doc * starts[None, :], axis=1)
    prefix_length = jnp.sum(pick_doc * prefix_lens[None, :], axis=1)
    return (document_index, inside_document, prefix_length)


class Ring:
    def __init__(self, count):
        self.count = count
        self.order = list(range(0, count, 2)) + list(range(count - 1, 0, -2))
        here = lax.axis_index("seq")
        self.place = jnp.where(here % 2 == 0, here // 2, count - 1 - here // 2)

    def index_at(self, place):
        place = lax.rem(place + self.count, self.count)
        return jnp.where(
            place < self.count // 2, 2 * place, 2 * (self.count - 1 - place) + 1
        )

    def shift(self, value, step):
        pairs = [
            (self.order[i], self.order[(i + step) % self.count]) for i in range(self.count)
        ]
        return lax.ppermute(value, "seq", pairs)

    def gather(self, value):
        got = [None] * self.count
        got[0] = value
        right = left = value
        for step in range(1, self.count // 2 + 1):
            right = self.shift(right, 1)
            got[step] = right
            if step < self.count - step:
                left = self.shift(left, -1)
                got[self.count - step] = left
        return got

    def scatter_sum(self, parts):
        half = self.count // 2
        total = parts[0].astype(F32)
        run = None
        for step in range(half, 0, -1):
            piece = parts[self.count - step].astype(F32)
            run = piece if run is None else piece + run.astype(F32)
            run = self.shift(run.astype(BF16), 1)
        back = None
        for step in range(half - 1, 0, -1):
            piece = parts[step].astype(F32)
            back = piece if back is None else piece + back.astype(F32)
            back = self.shift(back.astype(BF16), -1)
        total = total + run.astype(F32)
        return total if back is None else total + back.astype(F32)

    def in_order(self, got):
        filled = jnp.zeros((self.count,) + got[0].shape, got[0].dtype)
        for step, piece in enumerate(got):
            place = lax.rem(self.place - step + self.count, self.count)
            filled = lax.dynamic_update_index_in_dim(filled, piece, place, axis=0)
        return filled

    def exchange(self, pieces):
        got = []
        for step in range(self.count):
            mine = lax.dynamic_index_in_dim(
                pieces, self.index_at(self.place + step), axis=0, keepdims=False
            )
            got.append(mine if step == 0 else self.shift(mine, step))
        return got


def swap(value, axis):
    return lax.ppermute(value, axis, [(0, 1), (1, 0)])


def pair_sum(value):
    low = value.astype(BF16)
    return low.astype(F32) + swap(low, "tp").astype(F32)


def sum_all(value, seq_count):
    value = value + swap(value, "exp")
    step = 1
    while step < seq_count:
        value = value + lax.ppermute(value, "seq", [(i, i ^ step) for i in range(seq_count)])
        step *= 2
    return value


def slots_of(routes, experts):
    rows = routes.shape[-2]
    chosen = jnp.sum(
        (routes[..., None] == jnp.arange(experts, dtype=jnp.int32)).astype(F32), axis=-2
    )
    lower = jnp.tril(jnp.ones((rows, rows), BF16), -1)
    earlier = jnp.einsum(
        "st,...te->...se", lower, chosen.astype(BF16), preferred_element_type=F32
    )
    return chosen, earlier


def place_rows(chosen, earlier):
    slots = jnp.where(chosen > 0, earlier, -1.0).astype(jnp.int32)
    slots = jnp.swapaxes(slots, -1, -2)
    return (
        slots[..., :, None, :] == jnp.arange(CAP, dtype=jnp.int32)[:, None]
    ).astype(BF16)


def wgrad_kernel(count, *refs):
    hid_refs, pre_refs = refs[:count], refs[count : 2 * count]
    act_ref, out_ref, gate_ref, up_ref, down_ref = refs[2 * count :]
    hid = jnp.concatenate([ref[0] for ref in hid_refs], axis=0)
    pre = jnp.concatenate([ref[0] for ref in pre_refs], axis=0)
    units = hid.shape[1]
    width = act_ref.shape[-1]
    act = act_ref[...].reshape(hid.shape[0], width)
    out = out_ref[...].reshape(hid.shape[0], width)
    both = dot_rows(act, pre)
    gate_ref[0] = both[:, :units]
    up_ref[0] = both[:, units:]
    down_ref[0] = dot_rows(hid, out)


def expert_wgrads(hid, pre, act, out):
    count = len(hid)
    local_experts, rows, units = hid[0].shape
    seq_count, packs, _, cap, width = act.shape

    def by_expert(height, columns):
        return pl.BlockSpec((1, height, columns), lambda e: (e, 0, 0))

    rows_spec = pl.BlockSpec((seq_count, packs, 1, cap, width), lambda e: (0, 0, e, 0, 0))
    return pl.pallas_call(
        lambda *refs: wgrad_kernel(count, *refs),
        grid=(local_experts,),
        in_specs=[by_expert(rows, units)] * count
        + [by_expert(rows, 2 * units)] * count
        + [rows_spec] * 2,
        out_specs=[by_expert(width, units)] * 2 + [by_expert(units, width)],
        out_shape=[jax.ShapeDtypeStruct((local_experts, width, units), F32)] * 2
        + [jax.ShapeDtypeStruct((local_experts, units, width), F32)],
        cost_estimate=pl.CostEstimate(
            flops=6 * local_experts * count * rows * units * width,
            bytes_accessed=40_000_000,
            transcendentals=0,
        ),
        name="expert_wgrads",
    )(*hid, *pre, act, out)


def per_device(
    tokens,
    targets,
    attn_gain,
    wq,
    wk,
    wv,
    wo,
    moe_gain,
    router,
    w_gate,
    w_up,
    w_down,
    routes,
    lengths,
    prefix,
):
    rows_dev, model_width = tokens.shape
    exp_count = lax.axis_size("exp")
    seq_count = lax.axis_size("seq")
    exp_at = lax.axis_index("exp")
    seq_at = lax.axis_index("seq")
    ring = Ring(seq_count)
    pack_len = rows_dev * seq_count
    heads_q = wq.shape[1] // HEAD_SIZE
    heads_kv = wk.shape[1] // HEAD_SIZE
    kv_width = heads_kv * HEAD_SIZE
    repeat_heads = heads_q // heads_kv
    experts = router.shape[1]
    local_experts, _, units = w_gate.shape
    slice_width = model_width // seq_count
    scaling = 1.0 / math.sqrt(HEAD_SIZE)
    prefix_eff = jnp.minimum(prefix, lengths - 1)
    doc_lengths = lengths[exp_at]
    prefix_lens = prefix_eff[exp_at]
    block_at = ring.index_at(ring.place - jnp.arange(seq_count, dtype=jnp.int32))
    key_place = (
        block_at[:, None] * rows_dev + jnp.arange(rows_dev, dtype=jnp.int32)[None, :]
    ).reshape(pack_len)
    key_doc, key_local = doc_layout(doc_lengths, prefix_lens, key_place)[:2]
    query_place = seq_at * rows_dev + jnp.arange(rows_dev, dtype=jnp.int32)
    query_doc, query_local, query_limit = doc_layout(doc_lengths, prefix_lens, query_place)
    loss_count = jnp.sum(lengths - prefix_eff).astype(F32)
    factor = rows_dev * exp_count * seq_count / loss_count
    loss_mask = (query_local >= query_limit).astype(F32)
    frequency = jnp.exp(
        jnp.arange(HEAD_SIZE // 2, dtype=F32) * (-2.0 * math.log(10000.0) / HEAD_SIZE)
    )
    angles = query_local.astype(F32)[:, None, None] * frequency[None, None, :]
    cosine = jnp.cos(angles)
    sine_tab = jnp.sin(angles)

    x_full = tokens.astype(F32)
    inv_first = lax.rsqrt(jnp.mean(x_full * x_full, axis=1, keepdims=True) + eps)
    norm_first = x_full * inv_first
    first_activation = (attn_gain * norm_first).astype(BF16)
    key_matrix = jnp.dot(first_activation, wk, preferred_element_type=F32).reshape(
        rows_dev, heads_kv, HEAD_SIZE
    )
    key_matrix = rotate(key_matrix, cosine, sine_tab, 1.0).astype(BF16).reshape(rows_dev, kv_width)
    value_matrix = jnp.dot(first_activation, wv, preferred_element_type=F32).astype(BF16)
    both = jnp.concatenate(ring.gather(jnp.concatenate([key_matrix, value_matrix], axis=1)))
    query_matrix = jnp.dot(first_activation, wq, preferred_element_type=F32).reshape(
        rows_dev, heads_q, HEAD_SIZE
    )
    query_matrix = rotate(query_matrix, cosine, sine_tab, 1.0).astype(BF16)
    route_pair = jnp.concatenate([routes, swap(routes, "exp")], axis=1).astype(BF16)
    route_pad = 128 - route_pair.shape[1]
    first_got = ring.gather(
        jnp.concatenate([first_activation, jnp.pad(route_pair, ((0, 0), (0, route_pad)))], axis=1)
    )
    route_all = jnp.stack([got[:, model_width:] for got in first_got])
    route_all = route_all[..., : exp_count * routes.shape[1]].astype(jnp.int32)
    route_all = jnp.swapaxes(
        route_all.reshape(seq_count, rows_dev, exp_count, routes.shape[1]), 1, 2
    )
    first_all = ring.in_order([got[:, :model_width] for got in first_got])
    first_other = swap(first_all, "exp")

    key_all = both[:, :kv_width].reshape(pack_len, heads_kv, HEAD_SIZE)
    value_all = both[:, kv_width:].reshape(pack_len, heads_kv, HEAD_SIZE)
    query_heads = query_matrix.reshape(rows_dev, heads_kv, repeat_heads, HEAD_SIZE)
    allowed = (query_doc[:, None] == key_doc[None, :]) & (
        (key_place[None, :] <= query_place[:, None]) | (key_local[None, :] < query_limit[:, None])
    )
    scores = jnp.einsum("qgrd,kgd->grqk", query_heads, key_all, preferred_element_type=F32)
    scores = jnp.where(allowed, scores * scaling, neg_big)
    row_peak = jnp.max(scores, axis=-1, keepdims=True)
    probs = jnp.exp(scores - row_peak)
    probs = probs / jnp.sum(probs, axis=-1, keepdims=True)
    probs_low = probs.astype(BF16)
    attended_heads = jnp.einsum(
        "grqk,kgd->qgrd", probs_low, value_all, preferred_element_type=F32
    )
    attended_low = attended_heads.reshape(rows_dev, heads_q * HEAD_SIZE).astype(BF16)
    attn_out = pair_sum(jnp.dot(attended_low, wo, preferred_element_type=F32))

    hidden_one = x_full + attn_out
    inv_second = lax.rsqrt(jnp.mean(hidden_one * hidden_one, axis=1, keepdims=True) + eps)
    norm_second = hidden_one * inv_second
    act_second = (moe_gain * norm_second).astype(BF16)
    act_pair = jnp.stack([act_second, swap(act_second, "exp")])
    chosen_pair, earlier_pair = slots_of(
        jnp.swapaxes(
            route_pair.astype(jnp.int32).reshape(rows_dev, exp_count, routes.shape[1]), 0, 1
        ),
        experts,
    )
    logits = jnp.einsum("ptd,de->pte", act_pair, router, preferred_element_type=F32)
    logits = jnp.where(chosen_pair > 0, logits, neg_big)
    grown = jnp.where(
        chosen_pair > 0, jnp.exp(logits - jnp.max(logits, axis=-1, keepdims=True)), 0.0
    )
    gates = grown / jnp.sum(grown, axis=-1, keepdims=True)

    def own_experts(value):
        return lax.dynamic_slice_in_dim(value, exp_at * local_experts, local_experts, axis=-1)

    spots = place_rows(own_experts(chosen_pair), own_experts(earlier_pair))
    row_gate = jnp.einsum(
        "pect,pte->epc", spots.astype(F32), own_experts(gates), precision=lax.Precision.HIGHEST
    ).reshape(local_experts, exp_count * CAP, 1)

    def to_rows(value):
        rows = jnp.einsum("pect,ptd->epcd", spots, value, preferred_element_type=F32)
        return rows.astype(BF16).reshape(local_experts, exp_count * CAP, model_width)

    def to_tokens(rows):
        rows = rows.reshape(local_experts, exp_count, CAP, model_width)
        part = jnp.einsum("pect,epcd->ptd", spots, rows, preferred_element_type=F32)
        return part

    arrived = to_rows(act_pair)
    gate_pre = jnp.einsum("ecd,edf->ecf", arrived, w_gate, preferred_element_type=F32)
    up_pre = jnp.einsum("ecd,edf->ecf", arrived, w_up, preferred_element_type=F32)
    sigma_gate = jax.nn.sigmoid(gate_pre)
    swish_gate = gate_pre * sigma_gate
    inner_act = (swish_gate * up_pre).astype(BF16)
    gated_act = (row_gate * inner_act.astype(F32)).astype(BF16)
    gather_expert_rows = seq_count <= GATHER_MAX
    if gather_expert_rows:
        hid_got = ring.gather(gated_act)
    partial_out = jnp.einsum(
        "ecf,efd->ecd", inner_act, w_down, preferred_element_type=F32
    ).astype(BF16)
    moe_part = to_tokens((row_gate * partial_out.astype(F32)).astype(BF16))
    moe_part = moe_part[0] + swap(moe_part[1].astype(BF16), "exp").astype(F32)
    moe_out = pair_sum(moe_part)
    layer_out = hidden_one + moe_out

    out_grad = loss_mask[:, None] * (layer_out - targets.astype(F32)) * factor
    out_low = out_grad.astype(BF16)
    out_pair = jnp.stack([out_low, swap(out_low, "exp")])
    grad_rows = to_rows(out_pair)
    inner_grad = jnp.einsum("ecd,efd->ecf", grad_rows, w_down, preferred_element_type=F32)
    row_sens = jnp.sum(inner_act.astype(F32) * inner_grad, axis=-1)
    inner_grad = inner_grad * row_gate
    gate_rows = (inner_grad * up_pre * sigma_gate * (1.0 + gate_pre * (1.0 - sigma_gate))).astype(
        BF16
    )
    up_rows = (inner_grad * swish_gate).astype(BF16)
    if gather_expert_rows:
        gate_up = jnp.concatenate([gate_rows, up_rows], axis=-1)
        pre_got = ring.gather(gate_up)
    back_rows = jnp.einsum("ecf,edf->ecd", gate_rows, w_gate, preferred_element_type=F32)
    back_rows = (
        back_rows + jnp.einsum("ecf,edf->ecd", up_rows, w_up, preferred_element_type=F32)
    ).astype(BF16)
    back_part = to_tokens(back_rows)
    sens_part = jnp.einsum(
        "pect,epc->pte",
        spots.astype(F32),
        row_sens.reshape(local_experts, exp_count, CAP),
        precision=lax.Precision.HIGHEST,
    )
    sens_part = lax.dynamic_update_slice_in_dim(
        jnp.zeros((exp_count, rows_dev, 128), F32), sens_part, exp_at * local_experts, axis=2
    )
    back_part = jnp.concatenate([back_part, sens_part], axis=2)
    back_part = back_part[0] + swap(back_part[1].astype(BF16), "exp").astype(F32)
    back_sum = pair_sum(back_part)
    moe_in_grad = back_sum[:, :model_width]
    gate_sens = back_sum[:, model_width : model_width + experts]
    own_gates = gates[0]
    centered = own_gates * (gate_sens - jnp.sum(own_gates * gate_sens, axis=1, keepdims=True))
    logit_grad = centered.astype(BF16)
    router_wgrad = dot_rows(logit_grad, act_second)
    act_second_grad = moe_in_grad + dot_cols(logit_grad, router)
    scaled_second = moe_gain * act_second_grad
    hidden_grad = out_grad + inv_second * (
        scaled_second - norm_second * jnp.mean(scaled_second * norm_second, axis=1, keepdims=True)
    )
    moe_gain_grad = jnp.sum(act_second_grad * norm_second, axis=0)
    hidden_low = hidden_grad.astype(BF16)

    grad_heads = (
        dot_cols(hidden_low, wo)
        .astype(BF16)
        .reshape(rows_dev, heads_kv, repeat_heads, HEAD_SIZE)
    )
    delta_rows = jnp.transpose(
        jnp.sum(grad_heads.astype(F32) * attended_heads, axis=-1), (1, 2, 0)
    )
    prob_grad = jnp.einsum("qgrd,kgd->grqk", grad_heads, value_all, preferred_element_type=F32)
    score_grad = (probs * (prob_grad - delta_rows[..., None])).astype(BF16)
    query_grad = jnp.einsum("grqk,kgd->qgrd", score_grad, key_all, preferred_element_type=F32)
    key_parts = (
        jnp.einsum("grqk,qgrd->kgd", score_grad, query_heads, preferred_element_type=F32) * scaling
    )
    value_parts = jnp.einsum("grqk,qgrd->kgd", probs_low, grad_heads, preferred_element_type=F32)
    both_parts = jnp.concatenate(
        [
            key_parts.reshape(seq_count, rows_dev, kv_width),
            value_parts.reshape(seq_count, rows_dev, kv_width),
        ],
        axis=2,
    ).astype(BF16)
    both_sum = ring.scatter_sum([both_parts[i] for i in range(seq_count)])
    query_grad = (
        rotate(query_grad.reshape(rows_dev, heads_q, HEAD_SIZE) * scaling, cosine, sine_tab, -1.0)
        .astype(BF16)
        .reshape(rows_dev, heads_q * HEAD_SIZE)
    )
    key_grad = (
        rotate(
            both_sum[:, :kv_width].reshape(rows_dev, heads_kv, HEAD_SIZE), cosine, sine_tab, -1.0
        )
        .astype(BF16)
        .reshape(rows_dev, kv_width)
    )
    value_grad = both_sum[:, kv_width:].astype(BF16)
    first_part = dot_cols(query_grad, wq) + dot_cols(key_grad, wk) + dot_cols(value_grad, wv)
    act_first_grad = pair_sum(first_part)
    scaled_first = attn_gain * act_first_grad
    input_grad = hidden_grad + inv_first * (
        scaled_first - norm_first * jnp.mean(scaled_first * norm_first, axis=1, keepdims=True)
    )
    attn_gain_grad = jnp.sum(act_first_grad * norm_first, axis=0)
    small_sum = sum_all(
        jnp.concatenate([router_wgrad, moe_gain_grad[None], attn_gain_grad[None]]), seq_count
    )

    def over_tokens(first_own, first_oth, second_own, second_oth):
        def flat(value):
            return value.reshape(pack_len, value.shape[-1])

        return dot_rows(flat(first_own), flat(second_own)) + dot_rows(
            flat(first_oth), flat(second_oth)
        )

    query_width = heads_q * HEAD_SIZE
    hidden_all = ring.in_order(ring.gather(jnp.concatenate([attended_low, hidden_low], axis=1)))
    hidden_other = swap(hidden_all, "exp")
    wo_wgrad = over_tokens(
        hidden_all[..., :query_width],
        hidden_other[..., :query_width],
        hidden_all[..., query_width:],
        hidden_other[..., query_width:],
    )
    grads_all = ring.in_order(
        ring.gather(jnp.concatenate([query_grad, key_grad, value_grad], axis=1))
    )
    grads_other = swap(grads_all, "exp")
    wq_wgrad = over_tokens(
        first_all, first_other, grads_all[..., :query_width], grads_other[..., :query_width]
    )
    wkv_wgrad = over_tokens(
        first_all, first_other, grads_all[..., query_width:], grads_other[..., query_width:]
    )

    if gather_expert_rows:

        def pieces_of(value):
            return jnp.transpose(value.reshape(rows_dev, seq_count, slice_width), (1, 0, 2))

        slices = jnp.concatenate([pieces_of(act_second), pieces_of(out_low)], axis=2)
        slices, _ = lax.optimization_barrier((slices, hidden_low))
        slices = jnp.stack(ring.exchange(slices))
        slices = jnp.stack([slices, swap(slices, "exp")], axis=1)

        chosen_all, earlier_all = slots_of(route_all, experts)
        spots_all = place_rows(own_experts(chosen_all), own_experts(earlier_all))

        def rows_of_all(value):
            rows = jnp.einsum("kpect,kptd->kpecd", spots_all, value, preferred_element_type=F32)
            return rows.astype(BF16)

        expert_sums = expert_wgrads(
            hid_got,
            pre_got,
            rows_of_all(slices[..., :slice_width]),
            rows_of_all(slices[..., slice_width:]),
        )
    else:

        def scattered(first, second, dim):
            grad = jnp.einsum("ecd,ecf->edf", first, second, preferred_element_type=F32)
            return lax.psum_scatter(
                grad.astype(BF16), "seq", scatter_dimension=dim, tiled=True
            ).astype(F32)

        expert_sums = [
            scattered(arrived, gate_rows, 1),
            scattered(arrived, up_rows, 1),
            scattered(gated_act, grad_rows, 2),
        ]
    return (
        layer_out,
        input_grad,
        small_sum[experts + 1],
        wq_wgrad,
        wkv_wgrad[:, :kv_width],
        wkv_wgrad[:, kv_width:],
        wo_wgrad,
        small_sum[experts],
        small_sum[:experts].T,
        expert_sums[0],
        expert_sums[1],
        expert_sums[2],
    )


def solution(mesh):
    return jax.shard_map(
        per_device,
        mesh=mesh,
        in_specs=(
            P(("exp", "seq"), None),
            P(("exp", "seq"), None),
            P(),
            P(None, "tp"),
            P(None, "tp"),
            P(None, "tp"),
            P("tp", None),
            P(),
            P(),
            P("exp", None, "tp"),
            P("exp", None, "tp"),
            P("exp", "tp", None),
            P(("exp", "seq"), None),
            P(),
            P(),
        ),
        out_specs=(
            P(("exp", "seq"), None),
            P(("exp", "seq"), None),
            P(),
            P(None, "tp"),
            P(None, "tp"),
            P(None, "tp"),
            P("tp", None),
            P(),
            P(),
            P("exp", "seq", "tp"),
            P("exp", "seq", "tp"),
            P("exp", "tp", "seq"),
        ),
        check_vma=False,
    )
```
